32 devices in a mesh: freq: 16 (over z, x, core), row: 2 (over y).
Axes of the slice: x: 2, y: 2, z: 4, core: 2. Of those that a mesh axis runs over, the one named last changes fastest.
Arguments:
- reflect_re: float32 [16, 1728, 1728], P('freq', 'row'), may hold values from -0.046875 to 0.046875
- reflect_im: float32 [16, 1728, 1728], P('freq', 'row'), may hold values from -0.046875 to 0.046875
- focus_re: float32 [16, 1728, 32], P('freq', 'row'), may hold values from -6 to 6
- focus_im: float32 [16, 1728, 32], P('freq', 'row'), may hold values from -6 to 6
- first_arrival: int32 [1728, 32], P('row'), may hold values from 4 to 15
Outputs:
- minus_re: float32 [16, 1728, 32], P('freq', 'row')
- minus_im: float32 [16, 1728, 32], P('freq', 'row')
- plus_re: float32 [16, 1728, 32], P('freq', 'row')
- plus_im: float32 [16, 1728, 32], P('freq', 'row')
The draws below stay inside these ranges and needn't reach their ends.
All inputs are finite; a program needn't handle non-finite values.
Results may differ from the reference program's by a relative error of at most 0.0001.
Values sent between devices are 32-bit elements; how exact they have to be, the bound alone decides.
No kernel may reach another device: no remote copies, remote signals or barrier semaphores. Data moves between devices by JAX's collectives and lax.ppermute only.
A program may use at most 128 MiB of HBM per device.

```python
import math
import jax
import jax.numpy as jnp
from jax import lax

NR = 1728
NP = 32
ITERS = 4
NF = 16
NT = 32


def with_ends(result, key, smallest, top_value):
    index_at = [jax.random.randint(jax.random.fold_in(key, axis), (), 0, length) for axis, length in enumerate(result.shape)]
    widest = result.shape.index(max(result.shape))
    next_to = index_at[:widest] + [(index_at[widest] + 1) % result.shape[widest]] + index_at[widest + 1:]
    return result.at[tuple(index_at)].set(smallest).at[tuple(next_to)].set(top_value)


def block_scale(key, dims, split, least, top_value):
    loudness, own = 1.0, jax.random.fold_in(key, 6)
    for position, parts in split:
        draws = jnp.exp(jax.random.uniform(jax.random.fold_in(own, position), (parts,), jnp.float32, least / len(split), top_value / len(split)))
        loudness = loudness * jnp.repeat(draws, dims[position] // parts).reshape([-1 if axis == position else 1 for axis in range(len(dims))])
    return loudness


def gaussian(own_key, extent, width, bound, split=(), held_as=jnp.bfloat16):
    entries = width * jax.random.normal(own_key, extent, jnp.float32)
    if split:
        entries = entries * block_scale(own_key, extent, split, -0.22, 0.18)
    return jnp.clip(entries, -bound, bound).astype(held_as)


def setup_inputs(seed: int = 0) -> dict:
    splits = jax.random.split(jax.random.key(seed), 6)
    reflect_re = gaussian(splits[0], (NF, NR, NR), (11 * NR) ** -0.5, 0.046875, ((0, 16), (1, 2)), jnp.float32)
    reflect_im = gaussian(splits[1], (NF, NR, NR), (11 * NR) ** -0.5, 0.046875, ((0, 16), (1, 2)), jnp.float32)
    focus_re = gaussian(splits[2], (NF, NR, NP), 1.0, 6.0, ((0, 16), (1, 2)), jnp.float32)
    focus_im = gaussian(splits[3], (NF, NR, NP), 1.0, 6.0, ((0, 16), (1, 2)), jnp.float32)
    first_arrival = with_ends(jax.random.randint(splits[4], (NR, NP), NT // 8, NT // 2), jax.random.fold_in(splits[4], 1), NT // 8, (NT // 2) - 1).astype(jnp.int32)
    return {"reflect_re": reflect_re, "reflect_im": reflect_im, "focus_re": focus_re, "focus_im": focus_im, "first_arrival": first_arrival}


def spectra(freq_count, time_count):
    freq_ids = jnp.arange(freq_count, dtype=jnp.int32)
    time_ids = jnp.arange(time_count, dtype=jnp.int32)
    phase_ids = (time_ids[:, None] * freq_ids[None, :]) % time_count
    angle = (2.0 * math.pi / time_count) * phase_ids.astype(jnp.float32)
    weight = jnp.where(freq_ids == 0, 1.0 / time_count, 2.0 / time_count).astype(jnp.float32)
    return jnp.cos(angle), jnp.sin(angle), weight


def reference(reflect_re, reflect_im, focus_re, focus_im, first_arrival):
    highest = lax.Precision.HIGHEST
    cosine, sine, weight = spectra(NF, NT)
    time_ids = jnp.arange(NT, dtype=jnp.int32)
    distance = jnp.minimum(time_ids, NT - time_ids)
    window = (distance[:, None, None] < first_arrival[None, :, :]).astype(jnp.float32)

    def apply(field_re, field_im, conjugate):
        first = jnp.einsum('fij,fjp->fip', reflect_re, field_re, precision=highest)
        second = jnp.einsum('fij,fjp->fip', reflect_im, field_im, precision=highest)
        third = jnp.einsum('fij,fjp->fip', reflect_re, field_im, precision=highest)
        fourth = jnp.einsum('fij,fjp->fip', reflect_im, field_re, precision=highest)
        if conjugate:
            return first + second, third - fourth
        return first - second, third + fourth

    def filtered(spec_re, spec_im):
        traces = jnp.einsum('tk,kip->tip', cosine * weight[None, :], spec_re, precision=highest)
        traces = traces - jnp.einsum('tk,kip->tip', sine * weight[None, :], spec_im, precision=highest)
        masked = traces * window
        out_re = jnp.einsum('tk,tip->kip', cosine, masked, precision=highest)
        out_im = -jnp.einsum('tk,tip->kip', sine, masked, precision=highest)
        return out_re, out_im

    plus_re, plus_im = focus_re, focus_im
    minus_re = jnp.zeros_like(focus_re)
    minus_im = jnp.zeros_like(focus_im)
    for section in range(ITERS):
        if section % 2 == 0:
            minus_re, minus_im = filtered(*apply(plus_re, plus_im, False))
        else:
            upd_re, upd_im = filtered(*apply(minus_re, minus_im, True))
            plus_re = focus_re + upd_re
            plus_im = focus_im + upd_im
    return minus_re, minus_im, plus_re, plus_im
```

```python
import functools
import math

import jax
import jax.numpy as jnp
import numpy as np
from jax import lax
from jax.experimental import pallas as pl
from jax.experimental.pallas import tpu as pltpu
from jax.sharding import PartitionSpec as P

ITERS = 4
VMEM = pltpu.VMEM
LANES = 128


def up(value, unit):
    return -(-value // unit) * unit


def split(value):
    high = value.astype(jnp.bfloat16)
    low = (value - high.astype(jnp.float32)).astype(jnp.bfloat16)
    return high, low


def rows_step(total, unit=16, most=128):
    return max(s for s in range(unit, most + 1, unit) if total % s == 0)


def prepare_body(shards, half, pad, row_ref, re_ref, im_ref, *outs):
    step = re_ref.shape[0]
    first = pl.program_id(0) * step
    rows = pl.ds(pl.multiple_of(first, step), step)
    for me in range(shards):

        @pl.when(row_ref[0] == me)
        def _():
            for part in range(shards):
                start = (me + part) % shards * half
                for which, ref in enumerate((re_ref, im_ref)):
                    piece = ref[:, start : start + half]
                    if pad > half:
                        zeros = jnp.zeros((step, pad - half), jnp.float32)
                        piece = jnp.concatenate([piece, zeros], axis=1)
                    high, low = split(piece)
                    columns = slice(which * pad, (which + 1) * pad)
                    outs[2 * part][rows, columns] = high
                    outs[2 * part + 1][rows, columns] = low


def prepare(row, reflect_re, reflect_im, shards):
    half, full = reflect_re.shape
    pad = up(half, LANES)
    step = rows_step(half)
    shape = jax.ShapeDtypeStruct((half, 2 * pad), jnp.bfloat16)
    block = pl.BlockSpec((step, full), lambda i: (i, 0))
    return pl.pallas_call(
        functools.partial(prepare_body, shards, half, pad),
        grid=(half // step,),
        in_specs=[pl.BlockSpec(memory_space=pltpu.SMEM), block, block],
        out_specs=[pl.BlockSpec(memory_space=VMEM)] * (2 * shards),
        out_shape=[shape] * (2 * shards),
        compiler_params=pltpu.CompilerParams(vmem_limit_bytes=24 << 20),
        cost_estimate=pl.CostEstimate(
            flops=8 * half * full, bytes_accessed=8 * half * full, transcendentals=0
        ),
        name="prepare",
    )(row, reflect_re, reflect_im)


def product_body(sign, points, has_base, has_acc, last, *refs):
    refs = list(refs)
    out_ref, wide = refs[-2], refs[-1]
    u_ref = refs.pop(0)
    groups, per, half = u_ref.shape
    rows = groups * per
    pad = wide.shape[1]
    base_ref = refs.pop(0) if has_base else None
    acc_ref = refs.pop(0) if has_acc else None
    high_ref, low_ref = refs[0], refs[1]
    if pad > half:
        wide[:, pad - LANES :] = jnp.zeros((rows, LANES), jnp.float32)
    for g in range(groups):
        value = u_ref[g]
        if has_base:
            value = value + base_ref[g]
        wide[g * per : (g + 1) * per, :half] = value
    u = wide[...]
    place = lax.broadcasted_iota(jnp.int32, u.shape, 0) % per
    ahead = pltpu.roll(u, rows - points, 0)
    behind = pltpu.roll(u, points, 0)
    turned = jnp.where(place < points, -ahead, behind)
    if sign < 0:
        turned = -turned
    u_high, u_low = split(u)
    t_high, t_low = split(turned)
    high = jnp.concatenate([u_high, t_high], axis=1)
    low = jnp.concatenate([u_low, t_low], axis=1)
    both = jnp.concatenate([high, low], axis=0)
    dims = (((1,), (1,)), ((), ()))
    one = lax.dot_general(both, high_ref[...], dims, preferred_element_type=jnp.float32)
    two = lax.dot_general(high, low_ref[...], dims, preferred_element_type=jnp.float32)
    total = one[:rows] + one[rows:] + two
    if has_acc:
        total = total + acc_ref[...]
    if last:
        for g in range(groups):
            out_ref[g] = total[g * per : (g + 1) * per]
    else:
        out_ref[...] = total


def product(u, base, acc, high, low, sign, points, last):
    groups, per, half = u.shape
    rows = groups * per
    pad = high.shape[1] // 2
    args = [u] + [x for x in (base, acc) if x is not None] + [high, low]
    out = (groups, per, half) if last else (rows, half)
    return pl.pallas_call(
        functools.partial(
            product_body, sign, points, base is not None, acc is not None, last
        ),
        in_specs=[pl.BlockSpec(memory_space=VMEM)] * len(args),
        out_specs=pl.BlockSpec(memory_space=VMEM),
        out_shape=jax.ShapeDtypeStruct(out, jnp.float32),
        scratch_shapes=[pltpu.VMEM((rows, pad), jnp.float32)],
        compiler_params=pltpu.CompilerParams(vmem_limit_bytes=24 << 20),
        cost_estimate=pl.CostEstimate(
            flops=16 * half * half * rows, bytes_accessed=8 * half * pad, transcendentals=0
        ),
        name="product",
    )(*args)


def window_tables(time_count, points):
    angle = 2.0 * np.pi / time_count * np.arange(time_count)
    table = np.concatenate(
        [
            np.repeat(np.cos(angle)[:, None], points, 1),
            np.repeat(-np.sin(angle)[:, None], points, 1),
        ],
        axis=1,
    )
    return np.repeat(table[:, :, None], LANES, 2).astype(np.float32)


def window_body(freqs, points, g_ref, arrival_ref, table_ref, out_ref):
    times = 2 * freqs
    per, length = g_ref.shape[1:]
    middle = times // 4
    for start in range(0, length, LANES):
        size = min(LANES, length - start)
        lanes = slice(start, start + size)
        place = lax.broadcasted_iota(jnp.int32, (per, size), 0)
        side = jnp.where(place < points, 1.0, -1.0).astype(jnp.float32)
        arrival = arrival_ref[:, lanes]

        def tab(t, k):
            return table_ref[t * k % times][:, :size]

        g = []
        for k in range(freqs):
            weight = (1.0 if k == 0 else 2.0) / times
            g.append(g_ref[k][:, lanes] * weight)
        plus, minus = [], []
        for t in range(middle + 1):
            even = functools.reduce(lambda a, b: a + b, [tab(t, k) * g[k] for k in range(0, freqs, 2)])
            odd = functools.reduce(lambda a, b: a + b, [tab(t, k) * g[k] for k in range(1, freqs, 2)])
            scale = 1.0 if t == 0 else 2.0
            near = jnp.where(t < arrival, (even + odd) * scale, 0.0)
            if t == middle:
                plus.append(near)
                minus.append(near)
                continue
            far = jnp.where(times // 2 - t < arrival, (even - odd) * scale, 0.0)
            plus.append(near + far)
            minus.append(near - far)
        for k in range(freqs):
            source = plus if k % 2 == 0 else minus
            out_ref[k, :, lanes] = functools.reduce(
                lambda a, b: a + b, [tab(t, k) * source[t] for t in range(middle + 1)]
            )


def window_small(g, arrival, points):
    freqs = g.shape[0]
    table = jnp.asarray(window_tables(2 * freqs, points))
    return pl.pallas_call(
        functools.partial(window_body, freqs, points),
        in_specs=[pl.BlockSpec(memory_space=VMEM)] * 3,
        out_specs=pl.BlockSpec(memory_space=VMEM),
        out_shape=jax.ShapeDtypeStruct(g.shape, jnp.float32),
        compiler_params=pltpu.CompilerParams(vmem_limit_bytes=8 << 20),
        cost_estimate=pl.CostEstimate(
            flops=2 * freqs * g.size, bytes_accessed=8 * g.size, transcendentals=0
        ),
        name="window",
    )(g, arrival, table)


def window_large(g, arrival, points):
    freqs, per, length = g.shape
    times = 2 * freqs
    highest = lax.Precision.HIGHEST
    count = times // 2 + 1
    angle = 2.0 * np.pi / times * (np.arange(count)[:, None] * np.arange(freqs)[None, :] % times)
    weight = np.where(np.arange(freqs) == 0, 1.0, 2.0) / times
    fold = np.where(np.arange(count) % (times // 2) == 0, 1.0, 2.0)[:, None]
    mask = (jnp.arange(count, dtype=jnp.int32)[:, None, None] < arrival[None, :points]).astype(jnp.float32)
    outs = []
    for basis, part in ((np.cos(angle), g[:, :points]), (-np.sin(angle), g[:, points:])):
        forth = jnp.asarray((basis * weight).astype(np.float32))
        back = jnp.asarray((basis * fold).astype(np.float32))
        traces = jnp.einsum("tk,kil->til", forth, part, precision=highest) * mask
        outs.append(jnp.einsum("tk,til->kil", back, traces, precision=highest))
    return jnp.concatenate(outs, axis=1)


def local(reflect_re, reflect_im, focus_re, focus_im, first_arrival):
    shards = lax.axis_size("row")
    owners = lax.axis_size("freq")
    _, half, count = focus_re.shape
    groups = math.gcd(owners, count)
    points = count // groups
    cuts = owners // groups
    row = lax.axis_index("row")
    owner = lax.axis_index("freq")

    def field(re, im):
        both = jnp.stack([re[0].T.reshape(groups, points, half), im[0].T.reshape(groups, points, half)], axis=1)
        return both.reshape(groups, 2 * points, half)

    def out(value):
        both = value.reshape(groups, 2, points, half)
        return [both[:, c].reshape(count, half).T[None] for c in range(2)]

    def to_owners(value):
        if cuts > 1:
            value = value.reshape(groups, 2 * points, cuts, half // cuts).swapaxes(1, 2)
        value = value.reshape(owners, 2 * points, half // cuts)
        return lax.all_to_all(value, "freq", 0, 0, tiled=True)

    def from_owners(value):
        value = lax.all_to_all(value, "freq", 0, 0, tiled=True)
        if cuts > 1:
            value = value.reshape(groups, cuts, 2 * points, half // cuts).swapaxes(1, 2)
        return value.reshape(groups, 2 * points, half)

    def shift(value, by):
        pairs = [(i, (i - by) % shards) for i in range(shards)]
        return lax.ppermute(value, "row", pairs)

    arrival = first_arrival.T.reshape(groups, points, cuts, half // cuts).swapaxes(1, 2)
    arrival = arrival.reshape(owners, points, half // cuts)
    arrival = lax.dynamic_index_in_dim(arrival, owner, 0, keepdims=False)
    arrival = jnp.concatenate([arrival, arrival], axis=0)
    window = window_small if owners <= 32 else window_large

    base = field(focus_re, focus_im)
    bases = [base] + [shift(base, by) for by in range(1, shards)]
    parts = prepare(row.reshape(1), reflect_re[0], reflect_im[0], shards)

    def apply(fields, adds, sign):
        acc = None
        for by in range(shards):
            add = adds[by] if adds is not None else None
            acc = product(fields[by], add, acc, parts[2 * by], parts[2 * by + 1], sign, points, by == shards - 1)
        return from_owners(window(to_owners(acc), arrival, points))

    fields, adds = bases, None
    minus = plus = None
    for section in range(ITERS):
        result = apply(fields, adds, 1 if section % 2 == 0 else -1)
        if section % 2 == 0:
            minus, adds = result, None
        else:
            plus, adds = result, bases
        if section < ITERS - 1:
            fields = [result] + [shift(result, by) for by in range(1, shards)]
    return tuple(out(minus) + out(plus + base))


def solution(mesh):
    spec = P("freq", "row", None)
    return jax.shard_map(
        local,
        mesh=mesh,
        in_specs=(spec, spec, spec, spec, P("row", None)),
        out_specs=(spec, spec, spec, spec),
        check_vma=False,
    )
```

```python
import functools
import math

import jax
import jax.numpy as jnp
import numpy as np
from jax import lax
from jax.experimental import pallas as pl
from jax.experimental.pallas import tpu as pltpu
from jax.sharding import PartitionSpec as P

ITERS = 4
VMEM = pltpu.VMEM
SMEM = pltpu.SMEM
LANES = 128


def up(value, unit):
    return -(-value // unit) * unit


def whole(space):
    return pl.BlockSpec(memory_space=space)


def split(value):
    high = value.astype(jnp.bfloat16)
    low = (value - high.astype(jnp.float32)).astype(jnp.bfloat16)
    return high, low


def prepare_body(bands, groups, row_ref, owner_ref, arrival_ref, *refs):
    re_ref, im_ref, high_ref, low_ref, own_ref, re_held, im_held, arrived = refs
    full = re_ref.shape[1]
    pairs = ((re_ref, re_held), (im_ref, im_held))
    copies = {}
    for at, (start, size) in enumerate(bands):
        for which, (source, held) in enumerate(pairs):
            rows = slice(start, start + size)
            copies[at, which] = pltpu.make_async_copy(
                source.at[rows], held.at[rows], arrived.at[at, which]
            )
            copies[at, which].start()
    points = own_ref.shape[0] // 2
    own = jnp.zeros(own_ref.shape, jnp.int32)
    for g in range(groups):
        mine = arrival_ref[g * points : (g + 1) * points]
        own = jnp.where(owner_ref[0] == g, jnp.concatenate([mine, mine], axis=0), own)
    own_ref[...] = own
    for at, (start, size) in enumerate(bands):
        for which, (_, held) in enumerate(pairs):
            copies[at, which].wait()
            for column in range(0, full, LANES):
                width = min(LANES, full - column)
                piece = held[start : start + size, column : column + width]
                high, low = split(piece.T)
                rows = slice(which * full + column, which * full + column + width)
                high_ref[rows, start : start + size] = high
                low_ref[rows, start : start + size] = low


def prepare(row, owner, arrival, reflect_re, reflect_im, groups):
    half, full = reflect_re.shape
    points = arrival.shape[0] // groups
    bands = [(start, min(LANES, half - start)) for start in range(0, half, LANES)]
    shape = jax.ShapeDtypeStruct((2 * full, half), jnp.bfloat16)
    return pl.pallas_call(
        functools.partial(prepare_body, bands, groups),
        in_specs=[whole(SMEM)] * 2 + [whole(VMEM)] + [whole(pltpu.HBM)] * 2,
        out_specs=[whole(VMEM)] * 3,
        out_shape=[shape] * 2 + [jax.ShapeDtypeStruct((2 * points, half), jnp.int32)],
        scratch_shapes=[
            pltpu.VMEM((half, full), jnp.float32),
            pltpu.VMEM((half, full), jnp.float32),
            pltpu.SemaphoreType.DMA((len(bands), 2)),
        ],
        compiler_params=pltpu.CompilerParams(vmem_limit_bytes=40 << 20),
        cost_estimate=pl.CostEstimate(
            flops=32 * half * full * LANES, bytes_accessed=8 * half * full, transcendentals=0
        ),
        name="prepare",
    )(row, owner, arrival, reflect_re, reflect_im)


def product_body(sign, points, shards, joined, adds, emits, *refs):
    refs = list(refs)
    row = refs.pop(0)[0]
    wide = refs.pop()
    field_ref = refs.pop(0) if joined else None
    bases = [refs.pop(0) for _ in range(2 * shards)] if adds else None
    high_ref, low_ref, out_ref = refs[:3]
    groups, per, half = out_ref.shape
    rows = groups * per
    full = shards * half

    def base(rows_in, place, part):
        chosen = bases[part][rows_in]
        for by in range(1, shards):
            here = (row + by) % shards == place
            chosen = jnp.where(here, bases[2 * by + part][rows_in], chosen)
        return chosen

    for g in range(groups):
        rows_in = slice(g * points, (g + 1) * points)
        for place in range(shards):
            value = None
            if adds:
                value = jnp.concatenate([base(rows_in, place, part) for part in range(2)], axis=0)
            if joined:
                field = field_ref[g * shards + place]
                value = field if value is None else field + value
            wide[g * per : (g + 1) * per, place * half : (place + 1) * half] = value
    if emits:
        for g in range(groups):
            value = field_ref[g * shards + row]
            rows_out = slice(g * points, (g + 1) * points)
            refs[3][rows_out] = value[:points]
            refs[4][rows_out] = value[points:]
    u = wide[...]
    place = lax.broadcasted_iota(jnp.int32, u.shape, 0) % per
    ahead = pltpu.roll(u, rows - points, 0)
    behind = pltpu.roll(u, points, 0)
    turned = jnp.where(place < points, -ahead, behind)
    if sign < 0:
        turned = -turned
    u_high, u_low = split(u)
    t_high, t_low = split(turned)

    def times(left, ref, start):
        return lax.dot_general(
            left,
            ref[start : start + full],
            (((1,), (0,)), ((), ())),
            preferred_element_type=jnp.float32,
        )

    one = times(jnp.concatenate([u_high, u_low], axis=0), high_ref, 0)
    one = one + times(jnp.concatenate([t_high, t_low], axis=0), high_ref, full)
    two = times(u_high, low_ref, 0) + times(t_high, low_ref, full)
    result = one[:rows] + one[rows:] + two
    for g in range(groups):
        out_ref[g] = result[g * per : (g + 1) * per, :half]


def product(row, field, bases, high, low, sign, points, groups, shards, emits):
    half = high.shape[1]
    rows = 2 * points * groups
    args = [row] + ([] if field is None else [field]) + bases + [high, low]
    shapes = [jax.ShapeDtypeStruct((groups, 2 * points, half), jnp.float32)]
    if emits:
        shapes += [jax.ShapeDtypeStruct((groups * points, half), jnp.float32)] * 2
    return pl.pallas_call(
        functools.partial(
            product_body, sign, points, shards, field is not None, bool(bases), emits
        ),
        in_specs=[whole(SMEM)] + [whole(VMEM)] * (len(args) - 1),
        out_specs=[whole(VMEM)] * len(shapes),
        out_shape=shapes,
        scratch_shapes=[pltpu.VMEM((rows, shards * half), jnp.float32)],
        compiler_params=pltpu.CompilerParams(vmem_limit_bytes=24 << 20),
        cost_estimate=pl.CostEstimate(
            flops=12 * rows * shards * half * half,
            bytes_accessed=8 * half * half * shards,
            transcendentals=0,
        ),
        name="product",
    )(*args)


def window_tables(time_count, points):
    angle = 2.0 * np.pi / time_count * np.arange(time_count)
    table = np.concatenate(
        [
            np.repeat(np.cos(angle)[:, None], points, 1),
            np.repeat(-np.sin(angle)[:, None], points, 1),
        ],
        axis=1,
    )
    return np.repeat(table[:, :, None], LANES, 2).astype(np.float32)


def add_all(values):
    return functools.reduce(lambda a, b: a + b, values)


def window_body(freqs, points, copies, g_ref, arrival_ref, table_ref, out_ref):
    times = 2 * freqs
    length = g_ref.shape[2]
    middle = times // 4
    for start in range(0, length, LANES):
        size = min(LANES, length - start)
        lanes = slice(start, start + size)
        arrival = arrival_ref[:, lanes]

        def tab(t, k):
            return table_ref[t * k % times][:, :size]

        g = []
        for k in range(freqs):
            weight = (1.0 if k == 0 else 2.0) / times
            g.append(g_ref[k][:, lanes] * weight)
        plus, minus = [], []
        for t in range(middle + 1):
            even = add_all([tab(t, k) * g[k] for k in range(0, freqs, 2)])
            odd = add_all([tab(t, k) * g[k] for k in range(1, freqs, 2)])
            scale = 1.0 if t == 0 else 2.0
            near = jnp.where(t < arrival, (even + odd) * scale, 0.0)
            if t == middle:
                plus.append(near)
                minus.append(near)
                continue
            far = jnp.where(times // 2 - t < arrival, (even - odd) * scale, 0.0)
            plus.append(near + far)
            minus.append(near - far)
        for k in range(freqs):
            source = plus if k % 2 == 0 else minus
            value = add_all([tab(t, k) * source[t] for t in range(middle + 1)])
            for copy in range(copies):
                out_ref[k * copies + copy, :, lanes] = value


def window_small(g, arrival, points, copies):
    freqs = g.shape[0]
    table = jnp.asarray(window_tables(2 * freqs, points))
    return pl.pallas_call(
        functools.partial(window_body, freqs, points, copies),
        in_specs=[whole(VMEM)] * 3,
        out_specs=whole(VMEM),
        out_shape=jax.ShapeDtypeStruct((freqs * copies,) + g.shape[1:], jnp.float32),
        compiler_params=pltpu.CompilerParams(vmem_limit_bytes=8 << 20),
        cost_estimate=pl.CostEstimate(
            flops=2 * freqs * g.size, bytes_accessed=8 * g.size, transcendentals=0
        ),
        name="window",
    )(g, arrival, table)


def window_large(g, arrival, points, copies):
    freqs = g.shape[0]
    times = 2 * freqs
    highest = lax.Precision.HIGHEST
    count = times // 2 + 1
    angle = 2.0 * np.pi / times * (np.arange(count)[:, None] * np.arange(freqs)[None, :] % times)
    weight = np.where(np.arange(freqs) == 0, 1.0, 2.0) / times
    fold = np.where(np.arange(count) % (times // 2) == 0, 1.0, 2.0)[:, None]
    steps = jnp.arange(count, dtype=jnp.int32)[:, None, None]
    mask = (steps < arrival[None, :points]).astype(jnp.float32)
    outs = []
    for basis, part in ((np.cos(angle), g[:, :points]), (-np.sin(angle), g[:, points:])):
        forth = jnp.asarray((basis * weight).astype(np.float32))
        back = jnp.asarray((basis * fold).astype(np.float32))
        traces = jnp.einsum("tk,kil->til", forth, part, precision=highest) * mask
        outs.append(jnp.einsum("tk,til->kil", back, traces, precision=highest))
    return jnp.repeat(jnp.concatenate(outs, axis=1), copies, axis=0)


def finish_body(points, value_ref, base_re_ref, base_im_ref, re_ref, im_ref):
    for g in range(value_ref.shape[0]):
        value = value_ref[g]
        rows = slice(g * points, (g + 1) * points)
        re_ref[rows] = value[:points] + base_re_ref[rows]
        im_ref[rows] = value[points:] + base_im_ref[rows]


def finish(value, base_re, base_im):
    points = value.shape[1] // 2
    return pl.pallas_call(
        functools.partial(finish_body, points),
        in_specs=[whole(VMEM)] * 3,
        out_specs=[whole(VMEM)] * 2,
        out_shape=[jax.ShapeDtypeStruct(base_re.shape, jnp.float32)] * 2,
        compiler_params=pltpu.CompilerParams(vmem_limit_bytes=8 << 20),
        name="finish",
    )(value, base_re, base_im)


def local(reflect_re, reflect_im, focus_re, focus_im, first_arrival):
    shards = lax.axis_size("row")
    owners = lax.axis_size("freq")
    _, half, count = focus_re.shape
    groups = math.gcd(owners, count)
    points = count // groups
    cuts = owners // groups
    row = lax.axis_index("row").reshape(1)
    owner = lax.axis_index("freq").reshape(1)

    def to_owners(value):
        if cuts > 1:
            value = value.reshape(groups, 2 * points, cuts, half // cuts).swapaxes(1, 2)
            value = value.reshape(owners, 2 * points, half // cuts)
        return lax.all_to_all(value, "freq", 0, 0, tiled=True)

    def from_owners(value, axes, copies):
        value = lax.all_to_all(value, axes, 0, 0, tiled=True)
        if cuts > 1:
            value = value.reshape(groups, cuts, copies, 2 * points, half // cuts)
            value = value.transpose(0, 2, 3, 1, 4)
        return value.reshape(groups * copies, 2 * points, half)

    def shift(value, by):
        return lax.ppermute(value, "row", [(i, (i - by) % shards) for i in range(shards)])

    window = window_small if owners <= 32 else window_large
    bases = [focus_re[0].T, focus_im[0].T]
    for by in range(1, shards):
        bases += [shift(part, by) for part in bases[:2]]
    high, low, own_arrival = prepare(
        row, owner // cuts, first_arrival.T, reflect_re[0], reflect_im[0], groups
    )
    if cuts > 1:
        size = half // cuts
        own_arrival = lax.dynamic_slice_in_dim(own_arrival, owner[0] % cuts * size, size, 1)

    field, adds = None, bases
    for section in range(ITERS):
        last = section == ITERS - 1
        sign = 1 if section % 2 == 0 else -1
        outs = product(row, field, adds, high, low, sign, points, groups, shards, last)
        if last:
            minus = outs[1:]
        copies = 1 if last else shards
        value = window(to_owners(outs[0]), own_arrival, points, copies)
        field = from_owners(value, "freq" if last else ("freq", "row"), copies)
        adds = bases if section % 2 == 1 else []
    plus = finish(field, *bases[:2])
    return tuple(part.T[None] for part in list(minus) + list(plus))


def solution(mesh):
    spec = P("freq", "row", None)
    return jax.shard_map(
        local,
        mesh=mesh,
        in_specs=(spec, spec, spec, spec, P("row", None)),
        out_specs=(spec, spec, spec, spec),
        check_vma=False,
    )
```

```python
import functools
import math

import jax
import jax.numpy as jnp
import numpy as np
from jax import lax
from jax.experimental import pallas as pl
from jax.experimental.pallas import tpu as pltpu
from jax.sharding import PartitionSpec as P

ITERS = 4
VMEM = pltpu.VMEM
SMEM = pltpu.SMEM
LANES = 128


def up(value, unit):
    return -(-value // unit) * unit


def whole(space):
    return pl.BlockSpec(memory_space=space)


def split(value):
    high = value.astype(jnp.bfloat16)
    low = (value - high.astype(jnp.float32)).astype(jnp.bfloat16)
    return high, low


def column_of(half, which, start):
    main = half // LANES * LANES
    return which * main + start if start < main else 2 * main + which * LANES


def columns_in_all(half):
    main = half // LANES * LANES
    return 2 * main + (2 * LANES if main < half else 0)


def prepare_body(bands, row_ref, owner_ref, re_ref, im_ref, high_ref, low_ref, re_held, im_held, arrived):
    half, full = re_ref.shape
    pairs = ((re_ref, re_held), (im_ref, im_held))
    copies = {}
    for at, (start, size) in enumerate(bands):
        for which, (source, held) in enumerate(pairs):
            rows = slice(start, start + size)
            copies[at, which] = pltpu.make_async_copy(
                source.at[rows], held.at[rows], arrived.at[at, which]
            )
            copies[at, which].start()
    for at, (start, size) in enumerate(bands):
        for which, (_, held) in enumerate(pairs):
            copies[at, which].wait()
            place = column_of(half, which, start)
            for column in range(0, full, LANES):
                rows = slice(column, min(column + LANES, full))
                high, low = split(held[start : start + size, rows].T)
                high_ref[rows, place : place + size] = high
                low_ref[rows, place : place + size] = low


def prepare(row, owner, reflect_re, reflect_im):
    half, full = reflect_re.shape
    bands = [(start, min(LANES, half - start)) for start in range(0, half, LANES)]
    shape = jax.ShapeDtypeStruct((full, columns_in_all(half)), jnp.bfloat16)
    return pl.pallas_call(
        functools.partial(prepare_body, bands),
        in_specs=[whole(SMEM)] * 2 + [whole(pltpu.HBM)] * 2,
        out_specs=[whole(VMEM)] * 2,
        out_shape=[shape] * 2,
        scratch_shapes=[
            pltpu.VMEM((half, full), jnp.float32),
            pltpu.VMEM((half, full), jnp.float32),
            pltpu.SemaphoreType.DMA((len(bands), 2)),
        ],
        compiler_params=pltpu.CompilerParams(vmem_limit_bytes=40 << 20),
        cost_estimate=pl.CostEstimate(
            flops=32 * half * full * LANES, bytes_accessed=8 * half * full, transcendentals=0
        ),
        name="prepare",
    )(row, owner, reflect_re, reflect_im)


def product_body(sign, points, shards, joined, adds, first, *refs):
    refs = list(refs)
    row = refs.pop(0)[0]
    wide = refs.pop()
    field_ref = refs.pop(0) if joined else None
    bases = [refs.pop(0) for _ in range(2 * shards)] if adds else None
    high_ref, low_ref = refs[:2]
    out_ref = refs[4] if first else refs[2]
    groups, per, half = out_ref.shape
    rows = groups * per

    def base(rows_in, place, part):
        chosen = bases[part][rows_in]
        for by in range(1, shards):
            here = (row + by) % shards == place
            chosen = jnp.where(here, bases[2 * by + part][rows_in], chosen)
        return chosen

    for g in range(groups):
        rows_in = slice(g * points, (g + 1) * points)
        for place in range(shards):
            value = None
            if adds:
                value = jnp.concatenate([base(rows_in, place, part) for part in range(2)], axis=0)
            if joined:
                field = field_ref[g * shards + place]
                value = field if value is None else field + value
            wide[g * per : (g + 1) * per, place * half : (place + 1) * half] = value
    if first:
        owner_ref, arrival_ref, own_ref = refs[2], refs[3], refs[5]
        own = jnp.zeros(own_ref.shape, jnp.int32)
        for g in range(groups):
            mine = arrival_ref[g * points : (g + 1) * points]
            own = jnp.where(owner_ref[0] == g, jnp.concatenate([mine, mine], axis=0), own)
        own_ref[...] = own
    u_high, u_low = split(wide[...])
    both = jnp.concatenate([u_high, u_low], axis=0)
    one = jnp.dot(both, high_ref[...], preferred_element_type=jnp.float32)
    two = jnp.dot(u_high, low_ref[...], preferred_element_type=jnp.float32)
    result = one[:rows] + one[rows:] + two
    main = half // LANES * LANES
    parts = []
    for which in range(2):
        pieces = [result[:, which * main : (which + 1) * main]]
        if main < half:
            start = column_of(half, which, main)
            pieces.append(result[:, start : start + half - main])
        parts.append(jnp.concatenate(pieces, axis=1))
    real, imaginary = parts
    place = lax.broadcasted_iota(jnp.int32, imaginary.shape, 0) % per
    ahead = pltpu.roll(imaginary, rows - points, 0)
    behind = pltpu.roll(imaginary, points, 0)
    turned = jnp.where(place < points, -ahead, behind)
    total = real + turned if sign > 0 else real - turned
    for g in range(groups):
        out_ref[g] = total[g * per : (g + 1) * per]


def product(row, field, bases, high, low, sign, points, groups, shards, half, extra):
    rows = 2 * points * groups
    args = [row] + ([] if field is None else [field]) + bases + [high, low] + extra
    spaces = [SMEM] + [VMEM] * (len(args) - 1)
    shapes = [jax.ShapeDtypeStruct((groups, 2 * points, half), jnp.float32)]
    if extra:
        spaces[-2] = SMEM
        shapes.append(jax.ShapeDtypeStruct((2 * points, half), jnp.int32))
    return pl.pallas_call(
        functools.partial(
            product_body, sign, points, shards, field is not None, bool(bases), bool(extra)
        ),
        in_specs=[whole(space) for space in spaces],
        out_specs=[whole(VMEM)] * len(shapes),
        out_shape=shapes,
        scratch_shapes=[pltpu.VMEM((rows, shards * half), jnp.float32)],
        compiler_params=pltpu.CompilerParams(vmem_limit_bytes=24 << 20),
        cost_estimate=pl.CostEstimate(
            flops=12 * rows * shards * half * half,
            bytes_accessed=8 * half * half * shards,
            transcendentals=0,
        ),
        name="product",
    )(*args)


def window_tables(time_count, points):
    angle = 2.0 * np.pi / time_count * np.arange(time_count)
    table = np.concatenate(
        [
            np.repeat(np.cos(angle)[:, None], points, 1),
            np.repeat(-np.sin(angle)[:, None], points, 1),
        ],
        axis=1,
    )
    table = np.concatenate([table, table], axis=1)
    return np.repeat(table[:, :, None], LANES, 2).astype(np.float32)


def add_all(values):
    return functools.reduce(lambda a, b: a + b, values)


def window_body(freqs, points, copies, g_ref, arrival_ref, table_ref, out_ref):
    times = 2 * freqs
    per, length = g_ref.shape[1:]
    middle = times // 4
    tiles = [slice(start, min(start + LANES, length)) for start in range(0, length, LANES)]
    stacks = [tiles[i : i + 2] for i in range(0, len(tiles) - 1, 2)]
    if sum(len(stack) for stack in stacks) < len(tiles):
        stacks.append(tiles[-1:])
    if len(stacks[-1]) == 2 and length % LANES:
        stacks[-1:] = [stacks[-1][:1], stacks[-1][1:]]
    for stack in stacks:
        size = stack[0].stop - stack[0].start
        height = per * len(stack)

        def stacked(read):
            pieces = [read(lanes) for lanes in stack]
            return pieces[0] if len(pieces) == 1 else jnp.concatenate(pieces, axis=0)

        def tab(t, k):
            return table_ref[t * k % times][:height, :size]

        arrival = stacked(lambda lanes: arrival_ref[:, lanes])
        g = []
        for k in range(freqs):
            weight = (1.0 if k == 0 else 2.0) / times
            g.append(stacked(lambda lanes: g_ref[k][:, lanes]) * weight)
        plus, minus = [], []
        for t in range(middle + 1):
            even = add_all([tab(t, k) * g[k] for k in range(0, freqs, 2)])
            odd = add_all([tab(t, k) * g[k] for k in range(1, freqs, 2)])
            scale = 1.0 if t == 0 else 2.0
            near = jnp.where(t < arrival, (even + odd) * scale, 0.0)
            if t == middle:
                plus.append(near)
                minus.append(near)
                continue
            far = jnp.where(times // 2 - t < arrival, (even - odd) * scale, 0.0)
            plus.append(near + far)
            minus.append(near - far)
        for k in range(freqs):
            source = plus if k % 2 == 0 else minus
            value = add_all([tab(t, k) * source[t] for t in range(middle + 1)])
            for at, lanes in enumerate(stack):
                for copy in range(copies):
                    out_ref[k * copies + copy, :, lanes] = value[at * per : (at + 1) * per]


def window_small(g, arrival, points, copies):
    freqs = g.shape[0]
    table = jnp.asarray(window_tables(2 * freqs, points))
    return pl.pallas_call(
        functools.partial(window_body, freqs, points, copies),
        in_specs=[whole(VMEM)] * 3,
        out_specs=whole(VMEM),
        out_shape=jax.ShapeDtypeStruct((freqs * copies,) + g.shape[1:], jnp.float32),
        compiler_params=pltpu.CompilerParams(vmem_limit_bytes=8 << 20),
        cost_estimate=pl.CostEstimate(
            flops=2 * freqs * g.size, bytes_accessed=8 * g.size, transcendentals=0
        ),
        name="window",
    )(g, arrival, table)


def window_large(g, arrival, points, copies):
    freqs = g.shape[0]
    times = 2 * freqs
    highest = lax.Precision.HIGHEST
    count = times // 2 + 1
    angle = 2.0 * np.pi / times * (np.arange(count)[:, None] * np.arange(freqs)[None, :] % times)
    weight = np.where(np.arange(freqs) == 0, 1.0, 2.0) / times
    fold = np.where(np.arange(count) % (times // 2) == 0, 1.0, 2.0)[:, None]
    steps = jnp.arange(count, dtype=jnp.int32)[:, None, None]
    mask = (steps < arrival[None, :points]).astype(jnp.float32)
    outs = []
    for basis, part in ((np.cos(angle), g[:, :points]), (-np.sin(angle), g[:, points:])):
        forth = jnp.asarray((basis * weight).astype(np.float32))
        back = jnp.asarray((basis * fold).astype(np.float32))
        traces = jnp.einsum("tk,kil->til", forth, part, precision=highest) * mask
        outs.append(jnp.einsum("tk,til->kil", back, traces, precision=highest))
    return jnp.repeat(jnp.concatenate(outs, axis=1), copies, axis=0)


def finish_body(points, shards, row_ref, minus_ref, update_ref, *refs):
    base_re_ref, base_im_ref, minus_re_ref, minus_im_ref, plus_re_ref, plus_im_ref = refs
    row = row_ref[0]
    for g in range(update_ref.shape[0]):
        rows = slice(g * points, (g + 1) * points)
        value = minus_ref[g * shards]
        for place in range(1, shards):
            value = jnp.where(row == place, minus_ref[g * shards + place], value)
        minus_re_ref[rows] = value[:points]
        minus_im_ref[rows] = value[points:]
        value = update_ref[g]
        plus_re_ref[rows] = value[:points] + base_re_ref[rows]
        plus_im_ref[rows] = value[points:] + base_im_ref[rows]


def finish(row, minus, update, base_re, base_im, shards):
    points = update.shape[1] // 2
    return pl.pallas_call(
        functools.partial(finish_body, points, shards),
        in_specs=[whole(SMEM)] + [whole(VMEM)] * 4,
        out_specs=[whole(VMEM)] * 4,
        out_shape=[jax.ShapeDtypeStruct(base_re.shape, jnp.float32)] * 4,
        compiler_params=pltpu.CompilerParams(vmem_limit_bytes=8 << 20),
        name="finish",
    )(row, minus, update, base_re, base_im)


def local(reflect_re, reflect_im, focus_re, focus_im, first_arrival):
    shards = lax.axis_size("row")
    owners = lax.axis_size("freq")
    _, half, count = focus_re.shape
    groups = math.gcd(owners, count)
    points = count // groups
    cuts = owners // groups
    row = lax.axis_index("row").reshape(1)
    owner = (lax.axis_index("freq") // cuts).reshape(1)

    def to_owners(value):
        if cuts > 1:
            value = value.reshape(groups, 2 * points, cuts, half // cuts).swapaxes(1, 2)
            value = value.reshape(owners, 2 * points, half // cuts)
        return lax.all_to_all(value, "freq", 0, 0, tiled=True)

    def from_owners(value, axes, copies):
        value = lax.all_to_all(value, axes, 0, 0, tiled=True)
        if cuts > 1:
            value = value.reshape(groups, cuts, copies, 2 * points, half // cuts)
            value = value.transpose(0, 2, 3, 1, 4)
        return value.reshape(groups * copies, 2 * points, half)

    def shift(value, by):
        return lax.ppermute(value, "row", [(i, (i - by) % shards) for i in range(shards)])

    window = window_small if owners <= 32 else window_large
    bases = [focus_re[0].T, focus_im[0].T]
    for by in range(1, shards):
        bases += [shift(part, by) for part in bases[:2]]
    high, low = prepare(row, owner, reflect_re[0], reflect_im[0])

    field, adds, extra = None, bases, [owner, first_arrival.T]
    for section in range(ITERS):
        last = section == ITERS - 1
        sign = 1 if section % 2 == 0 else -1
        outs = product(row, field, adds, high, low, sign, points, groups, shards, half, extra)
        if extra:
            own_arrival, extra = outs[1], []
            if cuts > 1:
                size = half // cuts
                start = lax.axis_index("freq") % cuts * size
                own_arrival = lax.dynamic_slice_in_dim(own_arrival, start, size, 1)
        copies = 1 if last else shards
        value = window(to_owners(outs[0]), own_arrival, points, copies)
        if last:
            minus = field
        field = from_owners(value, "freq" if last else ("freq", "row"), copies)
        adds = bases if section % 2 == 1 else []
    results = finish(row, minus, field, *bases[:2], shards)
    return tuple(part.T[None] for part in results)


def solution(mesh):
    spec = P("freq", "row", None)
    return jax.shard_map(
        local,
        mesh=mesh,
        in_specs=(spec, spec, spec, spec, P("row", None)),
        out_specs=(spec, spec, spec, spec),
        check_vma=False,
    )
```

```python
import functools
import math

import jax
import jax.numpy as jnp
import numpy as np
from jax import lax
from jax.experimental import pallas as pl
from jax.experimental.pallas import tpu as pltpu
from jax.sharding import PartitionSpec as P

ITERS = 4
VMEM = pltpu.VMEM
SMEM = pltpu.SMEM
LANES = 128
TILE = 256


def up(value, unit):
    return -(-value // unit) * unit


def whole(space):
    return pl.BlockSpec(memory_space=space)


def split(value):
    high = value.astype(jnp.bfloat16)
    low = (value - high.astype(jnp.float32)).astype(jnp.bfloat16)
    return high, low


def pieces_of(half):
    return [(start, min(TILE, half - start)) for start in range(0, half, TILE)]


def columns_of(half):
    whole_pieces = half // TILE * 2 * TILE
    rest = 4 * up(half % TILE, LANES)
    return [whole_pieces] * 2 + ([rest] if rest else [])


def prepare_body(bands, row_ref, owner_ref, re_ref, im_ref, *refs):
    *outs, re_held, im_held, arrived = refs
    half, full = re_ref.shape
    pairs = ((re_ref, re_held), (im_ref, im_held))
    copies = {}
    for at, (start, size) in enumerate(bands):
        for which, (source, held) in enumerate(pairs):
            rows = slice(start, start + size)
            copies[at, which] = pltpu.make_async_copy(
                source.at[rows], held.at[rows], arrived.at[at, which]
            )
            copies[at, which].start()
    for at, (start, size) in enumerate(bands):
        for which, (_, held) in enumerate(pairs):
            copies[at, which].wait()
            first = start // TILE * TILE
            if first + TILE <= half:
                place = 2 * first + which * TILE + start - first
                targets = [(outs[0], place), (outs[1], place)]
            else:
                width = up(half - first, LANES)
                place = which * width + start - first
                targets = [(outs[2], place), (outs[2], place + 2 * width)]
            for line in range(0, full, LANES):
                rows = slice(line, min(line + LANES, full))
                parts = split(held[start : start + size, rows].T)
                for (target, place), part in zip(targets, parts):
                    target[rows, place : place + size] = part


def prepare(row, owner, reflect_re, reflect_im):
    half, full = reflect_re.shape
    bands = [(start, min(LANES, half - start)) for start in range(0, half, LANES)]
    shapes = [jax.ShapeDtypeStruct((full, width), jnp.bfloat16) for width in columns_of(half)]
    return pl.pallas_call(
        functools.partial(prepare_body, bands),
        in_specs=[whole(SMEM)] * 2 + [whole(pltpu.HBM)] * 2,
        out_specs=[whole(VMEM)] * len(shapes),
        out_shape=shapes,
        scratch_shapes=[
            pltpu.VMEM((half, full), jnp.float32),
            pltpu.VMEM((half, full), jnp.float32),
            pltpu.SemaphoreType.DMA((len(bands), 2)),
        ],
        compiler_params=pltpu.CompilerParams(vmem_limit_bytes=40 << 20),
        cost_estimate=pl.CostEstimate(
            flops=32 * half * full * LANES, bytes_accessed=8 * half * full, transcendentals=0
        ),
        name="prepare",
    )(row, owner, reflect_re, reflect_im)


def product_body(sign, points, shards, first, adds, *refs):
    refs = list(refs)
    if first:
        row_ref, owner_ref, arrival_ref = refs[:3]
        bases, refs = refs[3 : 3 + 2 * shards], refs[3 + 2 * shards :]
        *weights, out_ref, own_ref, wide = refs
    else:
        field_ref = refs.pop(0)
        base_ref = refs.pop(0) if adds else None
        *weights, out_ref, wide = refs
    groups, per, half = out_ref.shape
    rows = groups * per
    if first:
        for row in range(shards):

            @pl.when(row_ref[0] == row)
            def _():
                for g in range(groups):
                    for by in range(shards):
                        start = (row + by) % shards * half
                        for part in range(2):
                            target = g * per + part * points
                            wide[target : target + points, start : start + half] = bases[
                                2 * by + part
                            ][g * points : (g + 1) * points]

        own = jnp.zeros(own_ref.shape, jnp.int32)
        for g in range(groups):
            mine = arrival_ref[g * points : (g + 1) * points]
            own = jnp.where(owner_ref[0] == g, jnp.concatenate([mine, mine], axis=0), own)
        own_ref[...] = own
    else:
        for g in range(groups):
            band = slice(g * per, (g + 1) * per)
            for place in range(shards):
                lanes = slice(place * half, (place + 1) * half)
                wide[band, lanes] = field_ref[g * shards + place]
    u = wide[...] + base_ref[...] if adds else wide[...]
    u_high, u_low = split(u)
    both = jnp.concatenate([u_high, u_low], axis=0)
    for start, size in pieces_of(half):
        width = up(size, LANES)
        if size == TILE:
            columns = slice(2 * start, 2 * start + 2 * TILE)
            one = jnp.dot(both, weights[0][:, columns], preferred_element_type=jnp.float32)
            two = jnp.dot(u_high, weights[1][:, columns], preferred_element_type=jnp.float32)
        else:
            one = jnp.dot(both, weights[2][...], preferred_element_type=jnp.float32)
            one, two = one[:, : 2 * width], one[:rows, 2 * width :]
        result = one[:rows] + one[rows:] + two
        real, imaginary = result[:, :size], result[:, width : width + size]
        place = lax.broadcasted_iota(jnp.int32, imaginary.shape, 0) % per
        ahead = pltpu.roll(imaginary, rows - points, 0)
        behind = pltpu.roll(imaginary, points, 0)
        turned = jnp.where(place < points, -ahead, behind)
        total = real + turned if sign > 0 else real - turned
        for g in range(groups):
            out_ref[g, :, start : start + size] = total[g * per : (g + 1) * per]


def product(before, base, after, sign, points, groups, shards, half):
    first = len(before) > 1
    rows = 2 * points * groups
    args = before + ([] if base is None else [base]) + after
    field = jax.ShapeDtypeStruct((rows, shards * half), jnp.float32)
    shapes = [jax.ShapeDtypeStruct((groups, 2 * points, half), jnp.float32)]
    if first:
        shapes += [jax.ShapeDtypeStruct((2 * points, half), jnp.int32), field]
    return pl.pallas_call(
        functools.partial(product_body, sign, points, shards, first, base is not None),
        in_specs=[whole(SMEM if first and at < 2 else VMEM) for at in range(len(args))],
        out_specs=[whole(VMEM)] * len(shapes),
        out_shape=shapes,
        scratch_shapes=[] if first else [pltpu.VMEM(field.shape, jnp.float32)],
        compiler_params=pltpu.CompilerParams(vmem_limit_bytes=24 << 20),
        cost_estimate=pl.CostEstimate(
            flops=12 * rows * shards * half * half,
            bytes_accessed=8 * half * half * shards,
            transcendentals=0,
        ),
        name="product",
    )(*args)


def window_tables(time_count, points):
    angle = 2.0 * np.pi / time_count * np.arange(time_count)
    table = np.concatenate(
        [
            np.repeat(np.cos(angle)[:, None], points, 1),
            np.repeat(-np.sin(angle)[:, None], points, 1),
        ],
        axis=1,
    )
    table = np.concatenate([table, table], axis=1)
    return np.repeat(table[:, :, None], LANES, 2).astype(np.float32)


def add_all(values):
    return functools.reduce(lambda a, b: a + b, values)


def window_body(freqs, points, copies, g_ref, arrival_ref, table_ref, out_ref):
    times = 2 * freqs
    per, length = g_ref.shape[1:]
    middle = times // 4
    tiles = [slice(start, min(start + LANES, length)) for start in range(0, length, LANES)]
    stacks = [tiles[i : i + 2] for i in range(0, len(tiles) - 1, 2)]
    if sum(len(stack) for stack in stacks) < len(tiles):
        stacks.append(tiles[-1:])
    if len(stacks[-1]) == 2 and length % LANES:
        stacks[-1:] = [stacks[-1][:1], stacks[-1][1:]]
    for stack in stacks:
        size = stack[0].stop - stack[0].start
        height = per * len(stack)

        def stacked(read):
            pieces = [read(lanes) for lanes in stack]
            return pieces[0] if len(pieces) == 1 else jnp.concatenate(pieces, axis=0)

        def tab(t, k):
            return table_ref[t * k % times][:height, :size]

        arrival = stacked(lambda lanes: arrival_ref[:, lanes])
        g = []
        for k in range(freqs):
            weight = (1.0 if k == 0 else 2.0) / times
            g.append(stacked(lambda lanes: g_ref[k][:, lanes]) * weight)
        plus, minus = [], []
        for t in range(middle + 1):
            even = add_all([tab(t, k) * g[k] for k in range(0, freqs, 2)])
            odd = add_all([tab(t, k) * g[k] for k in range(1, freqs, 2)])
            scale = 1.0 if t == 0 else 2.0
            near = jnp.where(t < arrival, (even + odd) * scale, 0.0)
            if t == middle:
                plus.append(near)
                minus.append(near)
                continue
            far = jnp.where(times // 2 - t < arrival, (even - odd) * scale, 0.0)
            plus.append(near + far)
            minus.append(near - far)
        for k in range(freqs):
            source = plus if k % 2 == 0 else minus
            value = add_all([tab(t, k) * source[t] for t in range(middle + 1)])
            for at, lanes in enumerate(stack):
                for copy in range(copies):
                    out_ref[k * copies + copy, :, lanes] = value[at * per : (at + 1) * per]


def window_small(g, arrival, points, copies):
    freqs = g.shape[0]
    table = jnp.asarray(window_tables(2 * freqs, points))
    return pl.pallas_call(
        functools.partial(window_body, freqs, points, copies),
        in_specs=[whole(VMEM)] * 3,
        out_specs=whole(VMEM),
        out_shape=jax.ShapeDtypeStruct((freqs * copies,) + g.shape[1:], jnp.float32),
        compiler_params=pltpu.CompilerParams(vmem_limit_bytes=8 << 20),
        cost_estimate=pl.CostEstimate(
            flops=2 * freqs * g.size, bytes_accessed=8 * g.size, transcendentals=0
        ),
        name="window",
    )(g, arrival, table)


def window_large(g, arrival, points, copies):
    freqs = g.shape[0]
    times = 2 * freqs
    highest = lax.Precision.HIGHEST
    count = times // 2 + 1
    angle = 2.0 * np.pi / times * (np.arange(count)[:, None] * np.arange(freqs)[None, :] % times)
    weight = np.where(np.arange(freqs) == 0, 1.0, 2.0) / times
    fold = np.where(np.arange(count) % (times // 2) == 0, 1.0, 2.0)[:, None]
    steps = jnp.arange(count, dtype=jnp.int32)[:, None, None]
    mask = (steps < arrival[None, :points]).astype(jnp.float32)
    outs = []
    for basis, part in ((np.cos(angle), g[:, :points]), (-np.sin(angle), g[:, points:])):
        forth = jnp.asarray((basis * weight).astype(np.float32))
        back = jnp.asarray((basis * fold).astype(np.float32))
        traces = jnp.einsum("tk,kil->til", forth, part, precision=highest) * mask
        outs.append(jnp.einsum("tk,til->kil", back, traces, precision=highest))
    return jnp.repeat(jnp.concatenate(outs, axis=1), copies, axis=0)


def finish_body(points, shards, row_ref, minus_ref, update_ref, *refs):
    base_re_ref, base_im_ref, minus_re_ref, minus_im_ref, plus_re_ref, plus_im_ref = refs
    row = row_ref[0]
    for g in range(update_ref.shape[0]):
        rows = slice(g * points, (g + 1) * points)
        value = minus_ref[g * shards]
        for place in range(1, shards):
            value = jnp.where(row == place, minus_ref[g * shards + place], value)
        minus_re_ref[rows] = value[:points]
        minus_im_ref[rows] = value[points:]
        value = update_ref[g]
        plus_re_ref[rows] = value[:points] + base_re_ref[rows]
        plus_im_ref[rows] = value[points:] + base_im_ref[rows]


def finish(row, minus, update, base_re, base_im, shards):
    points = update.shape[1] // 2
    shape = jax.ShapeDtypeStruct(base_re.shape, jnp.float32)
    return pl.pallas_call(
        functools.partial(finish_body, points, shards),
        in_specs=[whole(SMEM)] + [whole(VMEM)] * 4,
        out_specs=[whole(VMEM)] * 4,
        out_shape=[shape] * 4,
        compiler_params=pltpu.CompilerParams(vmem_limit_bytes=8 << 20),
        name="finish",
    )(row, minus, update, base_re, base_im)


def local(reflect_re, reflect_im, focus_re, focus_im, first_arrival):
    shards = lax.axis_size("row")
    owners = lax.axis_size("freq")
    _, half, count = focus_re.shape
    groups = math.gcd(owners, count)
    points = count // groups
    cuts = owners // groups
    row = lax.axis_index("row").reshape(1)
    owner = (lax.axis_index("freq") // cuts).reshape(1)

    def to_owners(value):
        if cuts > 1:
            value = value.reshape(groups, 2 * points, cuts, half // cuts).swapaxes(1, 2)
            value = value.reshape(owners, 2 * points, half // cuts)
        return lax.all_to_all(value, "freq", 0, 0, tiled=True)

    def from_owners(value, axes, copies):
        value = lax.all_to_all(value, axes, 0, 0, tiled=True)
        if cuts > 1:
            value = value.reshape(groups, cuts, copies, 2 * points, half // cuts)
            value = value.transpose(0, 2, 3, 1, 4)
        return value.reshape(groups * copies, 2 * points, half)

    def shift(value, by):
        return lax.ppermute(value, "row", [(i, (i - by) % shards) for i in range(shards)])

    window = window_small if owners <= 32 else window_large
    bases = [focus_re[0].T, focus_im[0].T]
    for by in range(1, shards):
        bases += [shift(part, by) for part in bases[:2]]
    weights = list(prepare(row, owner, reflect_re[0], reflect_im[0]))

    before, adds = [row, owner, first_arrival.T] + bases, None
    for section in range(ITERS):
        last = section == ITERS - 1
        sign = 1 if section % 2 == 0 else -1
        outs = product(before, adds, weights, sign, points, groups, shards, half)
        if section == 0:
            own_arrival, whole_base = outs[1:]
            if cuts > 1:
                size = half // cuts
                start = lax.axis_index("freq") % cuts * size
                own_arrival = lax.dynamic_slice_in_dim(own_arrival, start, size, 1)
        copies = 1 if last else shards
        value = window(to_owners(outs[0]), own_arrival, points, copies)
        if last:
            minus = before[0]
        before = [from_owners(value, "freq" if last else ("freq", "row"), copies)]
        adds = whole_base if section % 2 == 1 else None
    results = finish(row, minus, before[0], *bases[:2], shards)
    return tuple(part.T[None] for part in results)


def solution(mesh):
    spec = P("freq", "row", None)
    return jax.shard_map(
        local,
        mesh=mesh,
        in_specs=(spec, spec, spec, spec, P("row", None)),
        out_specs=(spec, spec, spec, spec),
        check_vma=False,
    )
```

```python
import functools
import math

import jax
import jax.numpy as jnp
import numpy as np
from jax import lax
from jax.experimental import pallas as pl
from jax.experimental.pallas import tpu as pltpu
from jax.sharding import PartitionSpec as P

ITERS = 4
VMEM = pltpu.VMEM
SMEM = pltpu.SMEM
LANES = 128
TILE = 256


def up(value, unit):
    return -(-value // unit) * unit


def whole(space):
    return pl.BlockSpec(memory_space=space)


def split(value):
    high = value.astype(jnp.bfloat16)
    low = (value - high.astype(jnp.float32)).astype(jnp.bfloat16)
    return high, low


def pieces_of(half):
    return [(start, min(TILE, half - start)) for start in range(0, half, TILE)]


def columns_of(half):
    whole_pieces = half // TILE * 2 * TILE
    rest = 4 * up(half % TILE, LANES)
    return [whole_pieces] * 2 + ([rest] if rest else [])


def prepare_body(bands, rest, row_ref, owner_ref, re_ref, im_ref, *refs):
    *outs, re_held, im_held, arrived = refs
    half, full = re_ref.shape
    pairs = ((re_ref, re_held), (im_ref, im_held))
    copies = {}
    for at, (start, size) in enumerate(bands):
        for which, (source, held) in enumerate(pairs):
            rows = slice(start, start + size)
            copies[at, which] = pltpu.make_async_copy(
                source.at[rows], held.at[rows], arrived.at[at, which]
            )
            copies[at, which].start()
    for at, (start, size) in enumerate(bands):
        for which, (_, held) in enumerate(pairs):
            copies[at, which].wait()
            first = start // TILE * TILE
            if not rest:
                place = 2 * first + which * TILE + start - first
                targets = [(outs[0], place), (outs[1], place)]
            else:
                width = up(half - first, LANES)
                place = which * width + start - first
                targets = [(outs[0], place), (outs[0], place + 2 * width)]
            for line in range(0, full, LANES):
                rows = slice(line, min(line + LANES, full))
                parts = split(held[start : start + size, rows].T)
                for (target, place), part in zip(targets, parts):
                    target[rows, place : place + size] = part


def prepare(row, owner, reflect_re, reflect_im, rest):
    half, full = reflect_re.shape
    edge = half // TILE * TILE
    span = range(edge, half, LANES) if rest else range(0, edge, LANES)
    bands = [(start, min(LANES, half - start)) for start in span]
    widths = columns_of(half)[2:] if rest else columns_of(half)[:2]
    shapes = [jax.ShapeDtypeStruct((full, width), jnp.bfloat16) for width in widths]
    return pl.pallas_call(
        functools.partial(prepare_body, bands, rest),
        in_specs=[whole(SMEM)] * 2 + [whole(pltpu.HBM)] * 2,
        out_specs=[whole(VMEM)] * len(shapes),
        out_shape=shapes,
        scratch_shapes=[
            pltpu.VMEM((half, full), jnp.float32),
            pltpu.VMEM((half, full), jnp.float32),
            pltpu.SemaphoreType.DMA((len(bands), 2)),
        ],
        compiler_params=pltpu.CompilerParams(vmem_limit_bytes=(48 if rest else 40) << 20),
        cost_estimate=pl.CostEstimate(
            flops=32 * half * full * LANES, bytes_accessed=8 * half * full, transcendentals=0
        ),
        name="prepare",
    )(row, owner, reflect_re, reflect_im)


def product_body(sign, points, shards, first, adds, *refs):
    refs = list(refs)
    if first:
        row_ref, owner_ref, arrival_ref = refs[:3]
        bases, refs = refs[3 : 3 + 2 * shards], refs[3 + 2 * shards :]
        *weights, out_ref, own_ref, wide = refs
    else:
        field_ref = refs.pop(0)
        base_ref = refs.pop(0) if adds else None
        *weights, out_ref, wide = refs
    groups, per, half = out_ref.shape
    rows = groups * per
    if first:
        for row in range(shards):

            @pl.when(row_ref[0] == row)
            def _():
                for g in range(groups):
                    for by in range(shards):
                        start = (row + by) % shards * half
                        for part in range(2):
                            target = g * per + part * points
                            wide[target : target + points, start : start + half] = bases[
                                2 * by + part
                            ][g * points : (g + 1) * points]

        own = jnp.zeros(own_ref.shape, jnp.int32)
        for g in range(groups):
            mine = arrival_ref[g * points : (g + 1) * points]
            own = jnp.where(owner_ref[0] == g, jnp.concatenate([mine, mine], axis=0), own)
        own_ref[...] = own
    else:
        for g in range(groups):
            band = slice(g * per, (g + 1) * per)
            for place in range(shards):
                lanes = slice(place * half, (place + 1) * half)
                wide[band, lanes] = field_ref[g * shards + place]
    u = wide[...] + base_ref[...] if adds else wide[...]
    u_high, u_low = split(u)
    both = jnp.concatenate([u_high, u_low], axis=0)
    for start, size in pieces_of(half):
        width = up(size, LANES)
        if size == TILE:
            columns = slice(2 * start, 2 * start + 2 * TILE)
            one = jnp.dot(both, weights[0][:, columns], preferred_element_type=jnp.float32)
            two = jnp.dot(u_high, weights[1][:, columns], preferred_element_type=jnp.float32)
        else:
            one = jnp.dot(both, weights[2][...], preferred_element_type=jnp.float32)
            one, two = one[:, : 2 * width], one[:rows, 2 * width :]
        result = one[:rows] + one[rows:] + two
        real, imaginary = result[:, :size], result[:, width : width + size]
        place = lax.broadcasted_iota(jnp.int32, imaginary.shape, 0) % per
        ahead = pltpu.roll(imaginary, rows - points, 0)
        behind = pltpu.roll(imaginary, points, 0)
        turned = jnp.where(place < points, -ahead, behind)
        total = real + turned if sign > 0 else real - turned
        for g in range(groups):
            out_ref[g, :, start : start + size] = total[g * per : (g + 1) * per]


def product(before, base, after, sign, points, groups, shards, half):
    first = len(before) > 1
    rows = 2 * points * groups
    args = before + ([] if base is None else [base]) + after
    field = jax.ShapeDtypeStruct((rows, shards * half), jnp.float32)
    shapes = [jax.ShapeDtypeStruct((groups, 2 * points, half), jnp.float32)]
    if first:
        shapes += [jax.ShapeDtypeStruct((2 * points, half), jnp.int32), field]
    return pl.pallas_call(
        functools.partial(product_body, sign, points, shards, first, base is not None),
        in_specs=[whole(SMEM if first and at < 2 else VMEM) for at in range(len(args))],
        out_specs=[whole(VMEM)] * len(shapes),
        out_shape=shapes,
        scratch_shapes=[] if first else [pltpu.VMEM(field.shape, jnp.float32)],
        compiler_params=pltpu.CompilerParams(vmem_limit_bytes=24 << 20),
        cost_estimate=pl.CostEstimate(
            flops=12 * rows * shards * half * half,
            bytes_accessed=8 * half * half * shards,
            transcendentals=0,
        ),
        name="product",
    )(*args)


def window_tables(time_count, points):
    angle = 2.0 * np.pi / time_count * np.arange(time_count)
    table = np.concatenate(
        [
            np.repeat(np.cos(angle)[:, None], points, 1),
            np.repeat(-np.sin(angle)[:, None], points, 1),
        ],
        axis=1,
    )
    table = np.concatenate([table, table], axis=1)
    return np.repeat(table[:, :, None], LANES, 2).astype(np.float32)


def add_all(values):
    return functools.reduce(lambda a, b: a + b, values)


def window_body(freqs, points, copies, g_ref, arrival_ref, table_ref, out_ref):
    times = 2 * freqs
    per, length = g_ref.shape[1:]
    middle = times // 4
    tiles = [slice(start, min(start + LANES, length)) for start in range(0, length, LANES)]
    stacks = [tiles[i : i + 2] for i in range(0, len(tiles) - 1, 2)]
    if sum(len(stack) for stack in stacks) < len(tiles):
        stacks.append(tiles[-1:])
    if len(stacks[-1]) == 2 and length % LANES:
        stacks[-1:] = [stacks[-1][:1], stacks[-1][1:]]
    for stack in stacks:
        size = stack[0].stop - stack[0].start
        height = per * len(stack)

        def stacked(read):
            pieces = [read(lanes) for lanes in stack]
            return pieces[0] if len(pieces) == 1 else jnp.concatenate(pieces, axis=0)

        def tab(t, k):
            return table_ref[t * k % times][:height, :size]

        arrival = stacked(lambda lanes: arrival_ref[:, lanes])
        g = []
        for k in range(freqs):
            weight = (1.0 if k == 0 else 2.0) / times
            g.append(stacked(lambda lanes: g_ref[k][:, lanes]) * weight)
        plus, minus = [], []
        for t in range(middle + 1):
            even = add_all([tab(t, k) * g[k] for k in range(0, freqs, 2)])
            odd = add_all([tab(t, k) * g[k] for k in range(1, freqs, 2)])
            scale = 1.0 if t == 0 else 2.0
            near = jnp.where(t < arrival, (even + odd) * scale, 0.0)
            if t == middle:
                plus.append(near)
                minus.append(near)
                continue
            far = jnp.where(times // 2 - t < arrival, (even - odd) * scale, 0.0)
            plus.append(near + far)
            minus.append(near - far)
        for k in range(freqs):
            source = plus if k % 2 == 0 else minus
            value = add_all([tab(t, k) * source[t] for t in range(middle + 1)])
            for at, lanes in enumerate(stack):
                for copy in range(copies):
                    out_ref[k * copies + copy, :, lanes] = value[at * per : (at + 1) * per]


def window_small(g, arrival, points, copies):
    freqs = g.shape[0]
    table = jnp.asarray(window_tables(2 * freqs, points))
    return pl.pallas_call(
        functools.partial(window_body, freqs, points, copies),
        in_specs=[whole(VMEM)] * 3,
        out_specs=whole(VMEM),
        out_shape=jax.ShapeDtypeStruct((freqs * copies,) + g.shape[1:], jnp.float32),
        compiler_params=pltpu.CompilerParams(vmem_limit_bytes=8 << 20),
        cost_estimate=pl.CostEstimate(
            flops=2 * freqs * g.size, bytes_accessed=8 * g.size, transcendentals=0
        ),
        name="window",
    )(g, arrival, table)


def window_large(g, arrival, points, copies):
    freqs = g.shape[0]
    times = 2 * freqs
    highest = lax.Precision.HIGHEST
    count = times // 2 + 1
    angle = 2.0 * np.pi / times * (np.arange(count)[:, None] * np.arange(freqs)[None, :] % times)
    weight = np.where(np.arange(freqs) == 0, 1.0, 2.0) / times
    fold = np.where(np.arange(count) % (times // 2) == 0, 1.0, 2.0)[:, None]
    steps = jnp.arange(count, dtype=jnp.int32)[:, None, None]
    mask = (steps < arrival[None, :points]).astype(jnp.float32)
    outs = []
    for basis, part in ((np.cos(angle), g[:, :points]), (-np.sin(angle), g[:, points:])):
        forth = jnp.asarray((basis * weight).astype(np.float32))
        back = jnp.asarray((basis * fold).astype(np.float32))
        traces = jnp.einsum("tk,kil->til", forth, part, precision=highest) * mask
        outs.append(jnp.einsum("tk,til->kil", back, traces, precision=highest))
    return jnp.repeat(jnp.concatenate(outs, axis=1), copies, axis=0)


def finish_body(points, shards, row_ref, minus_ref, update_ref, *refs):
    base_re_ref, base_im_ref, minus_re_ref, minus_im_ref, plus_re_ref, plus_im_ref = refs
    row = row_ref[0]
    for g in range(update_ref.shape[0]):
        rows = slice(g * points, (g + 1) * points)
        value = minus_ref[g * shards]
        for place in range(1, shards):
            value = jnp.where(row == place, minus_ref[g * shards + place], value)
        minus_re_ref[rows] = value[:points]
        minus_im_ref[rows] = value[points:]
        value = update_ref[g]
        plus_re_ref[rows] = value[:points] + base_re_ref[rows]
        plus_im_ref[rows] = value[points:] + base_im_ref[rows]


def finish(row, minus, update, base_re, base_im, shards):
    points = update.shape[1] // 2
    shape = jax.ShapeDtypeStruct(base_re.shape, jnp.float32)
    return pl.pallas_call(
        functools.partial(finish_body, points, shards),
        in_specs=[whole(SMEM)] + [whole(VMEM)] * 4,
        out_specs=[whole(VMEM)] * 4,
        out_shape=[shape] * 4,
        compiler_params=pltpu.CompilerParams(vmem_limit_bytes=8 << 20),
        name="finish",
    )(row, minus, update, base_re, base_im)


def local(reflect_re, reflect_im, focus_re, focus_im, first_arrival):
    shards = lax.axis_size("row")
    owners = lax.axis_size("freq")
    _, half, count = focus_re.shape
    groups = math.gcd(owners, count)
    points = count // groups
    cuts = owners // groups
    row = lax.axis_index("row").reshape(1)
    owner = (lax.axis_index("freq") // cuts).reshape(1)

    def to_owners(value):
        if cuts > 1:
            value = value.reshape(groups, 2 * points, cuts, half // cuts).swapaxes(1, 2)
            value = value.reshape(owners, 2 * points, half // cuts)
        return lax.all_to_all(value, "freq", 0, 0, tiled=True)

    def from_owners(value, axes, copies):
        value = lax.all_to_all(value, axes, 0, 0, tiled=True)
        if cuts > 1:
            value = value.reshape(groups, cuts, copies, 2 * points, half // cuts)
            value = value.transpose(0, 2, 3, 1, 4)
        return value.reshape(groups * copies, 2 * points, half)

    def shift(value, by):
        return lax.ppermute(value, "row", [(i, (i - by) % shards) for i in range(shards)])

    window = window_small if owners <= 32 else window_large
    bases = [focus_re[0].T, focus_im[0].T]
    moved = [shift(bases[0], by) for by in range(1, shards)]
    matrix = (reflect_re[0], reflect_im[0])
    left, held = [], bases[1]
    if half % TILE:
        left = list(prepare(row, owner, *matrix, True))
        held, left[0] = lax.optimization_barrier((held, left[0]))
    for by in range(1, shards):
        bases += [moved[by - 1], shift(held, by)]
    weights = list(prepare(row, owner, *matrix, False)) + left

    before, adds = [row, owner, first_arrival.T] + bases, None
    for section in range(ITERS):
        last = section == ITERS - 1
        sign = 1 if section % 2 == 0 else -1
        outs = product(before, adds, weights, sign, points, groups, shards, half)
        if section == 0:
            own_arrival, whole_base = outs[1:]
            if cuts > 1:
                size = half // cuts
                start = lax.axis_index("freq") % cuts * size
                own_arrival = lax.dynamic_slice_in_dim(own_arrival, start, size, 1)
        copies = 1 if last else shards
        value = window(to_owners(outs[0]), own_arrival, points, copies)
        if last:
            minus = before[0]
        before = [from_owners(value, "freq" if last else ("freq", "row"), copies)]
        adds = whole_base if section % 2 == 1 else None
    results = finish(row, minus, before[0], *bases[:2], shards)
    return tuple(part.T[None] for part in results)


def solution(mesh):
    spec = P("freq", "row", None)
    return jax.shard_map(
        local,
        mesh=mesh,
        in_specs=(spec, spec, spec, spec, P("row", None)),
        out_specs=(spec, spec, spec, spec),
        check_vma=False,
    )
```
